32 devices in a mesh: expert: 4 (over z), shard: 8 (over y, x, core).
Axes of the slice: x: 2, y: 2, z: 4, core: 2. Of those that a mesh axis runs over, the one named last changes fastest.
Arguments:
- master_gate: float32 [64, 2048, 1024], P('expert', 'shard'), may hold values from -0.1875 to 0.1875
- second_gate: float32 [64, 2048, 1024], P('expert', 'shard'), may hold values from -0.125 to 0.125
- master_up: float32 [64, 2048, 1024], P('expert', 'shard'), may hold values from -0.1875 to 0.1875
- second_up: float32 [64, 2048, 1024], P('expert', 'shard'), may hold values from -0.125 to 0.125
- mix_share: float32 [64], P('expert'), may hold values from 0.2 to 0.8
- router_weight: float32 [2048, 64], P('shard', 'expert'), may hold values from -0.125 to 0.125
- router_gain: float32 [2048], P('shard'), may hold values from 0.25 to 1.75
Outputs:
- final_gate: bfloat16 [64, 2048, 1024], P('expert', None, 'shard')
- final_up: bfloat16 [64, 2048, 1024], P('expert', None, 'shard')
- scale_gate: float32 [64, 1024], P('expert', 'shard')
- scale_up: float32 [64, 1024], P('expert', 'shard')
- serve_router: bfloat16 [2048, 64], replicated
The draws below stay inside these ranges and needn't reach their ends.
All inputs are finite; a program needn't handle non-finite values.
Results may differ from the reference program's by a relative error of at most 0.001.
Values may be sent and summed in bfloat16 or wider, within the bound.
A program may use at most 256 MiB of HBM per device.

```python
import jax
import jax.numpy as jnp

EXPERTS = 64
D_MODEL = 2048
D_EXPERT = 1024


def with_spikes(values, own_key, source, target, blocks, factor):
    def block_of(position):
        return (jnp.arange(values.shape[position]) // (values.shape[position] // blocks)).reshape((-1,) + (1,) * (values.ndim - 1 - position))

    first = jax.random.permutation(own_key, blocks)[block_of(target)]
    other_side = (block_of(target) + blocks // 2) % blocks
    return jnp.where((block_of(source) == first) | (block_of(source) == other_side), factor * values, values)


def block_scale(key, dims, cuts, low, top_value):
    factor_of, own = 1.0, jax.random.fold_in(key, 6)
    for axis_at, shards_of in cuts:
        draws = jnp.exp(jax.random.uniform(jax.random.fold_in(own, axis_at), (shards_of,), jnp.float32, low / len(cuts), top_value / len(cuts)))
        factor_of = factor_of * jnp.repeat(draws, dims[axis_at] // shards_of).reshape([-1 if axis == axis_at else 1 for axis in range(len(dims))])
    return factor_of


def normal_values(rng, extent, deviation, bound, shards=(), dtype=jnp.bfloat16):
    factor_of = block_scale(rng, extent, shards, -0.22, 0.18) if shards else 1.0
    array = jax.random.normal(rng, extent, jnp.float32) * deviation * factor_of
    return jnp.minimum(jnp.maximum(array, -bound), bound).astype(dtype)


def heavy_noise(rng, extent, spread, reach, pieces, heavy, dtype=jnp.bfloat16):
    drawn = spread * jax.random.normal(rng, extent, jnp.float32)
    if pieces:
        drawn = drawn * block_scale(rng, extent, pieces, -0.22, 0.18)
    return jnp.clip(with_spikes(drawn, jax.random.fold_in(rng, 3), *heavy), -reach, reach).astype(dtype)


def setup_inputs(seed: int = 0) -> dict:
    streams_of = jax.random.split(jax.random.key(seed), 8)
    master_gate = heavy_noise(streams_of[0], (EXPERTS, D_MODEL, D_EXPERT), D_MODEL ** -0.5, 0.1875, ((0, 4), (1, 8)), (1, 2, 8, 2.0), jnp.float32)
    second_gate = normal_values(streams_of[1], (EXPERTS, D_MODEL, D_EXPERT), D_MODEL ** -0.5, 0.125, ((0, 4), (1, 8)), jnp.float32)
    master_up = heavy_noise(streams_of[2], (EXPERTS, D_MODEL, D_EXPERT), D_MODEL ** -0.5, 0.1875, ((0, 4), (1, 8)), (1, 2, 8, 2.0), jnp.float32)
    second_up = normal_values(streams_of[3], (EXPERTS, D_MODEL, D_EXPERT), D_MODEL ** -0.5, 0.125, ((0, 4), (1, 8)), jnp.float32)
    mix_share = jnp.clip(0.2 + 0.6 * jax.random.uniform(streams_of[4], (EXPERTS,), jnp.float32) ** block_scale(streams_of[4], (EXPERTS,), ((0, 4),), -0.2, 0.2), 0.2, 0.8)
    router_weight = normal_values(streams_of[5], (D_MODEL, EXPERTS), D_MODEL ** -0.5, 0.125, ((0, 8), (1, 4)), jnp.float32)
    router_gain = jnp.clip(1.0 + 0.15 * jax.random.normal(streams_of[6], (D_MODEL,), jnp.float32), 0.25, 1.75)
    return {"master_gate": master_gate, "second_gate": second_gate, "master_up": master_up, "second_up": second_up, "mix_share": mix_share, "router_weight": router_weight, "router_gain": router_gain}


def reference(master_gate, second_gate, master_up, second_up, mix_share, router_weight, router_gain):
    merged_gate = mix_share[:, None, None] * master_gate + (1.0 - mix_share[:, None, None]) * second_gate
    merged_up = mix_share[:, None, None] * master_up + (1.0 - mix_share[:, None, None]) * second_up
    scale_gate = jnp.sum(jnp.abs(merged_gate), axis=1) / D_MODEL
    final_gate = (merged_gate / jnp.expand_dims(scale_gate, 1)).astype(jnp.bfloat16)
    scale_up = jnp.sum(jnp.abs(merged_up), axis=1) / D_MODEL
    final_up = (merged_up / jnp.expand_dims(scale_up, 1)).astype(jnp.bfloat16)
    serve_router = (router_weight * router_gain[:, None]).astype(jnp.bfloat16)
    return final_gate, final_up, scale_gate, scale_up, serve_router
```

```python
import functools

import jax
import jax.numpy as jnp
from jax import lax
from jax.experimental import pallas as pl
from jax.experimental.pallas import tpu as pltpu
from jax.sharding import PartitionSpec as P

LANES = 128
LOAD_SLOTS = 3
SUM_LAG = 1
SCALE_LAG = 1
KEPT = SUM_LAG + SCALE_LAG + 1


def plain(width, master_gate, second_gate, master_up, second_up, mix_share, router_weight, router_gain):
    share = mix_share[:, None, None]
    merged_gate = share * master_gate + (1.0 - share) * second_gate
    merged_up = share * master_up + (1.0 - share) * second_up
    total_gate, total_up = lax.psum(
        (jnp.sum(jnp.abs(merged_gate), axis=1), jnp.sum(jnp.abs(merged_up), axis=1)), "shard"
    )
    rows = master_gate.shape[1] * lax.axis_size("shard")
    finals, scales = [], []
    for merged, total in ((merged_gate, total_gate), (merged_up, total_up)):
        scale = total / rows
        narrow = (merged / jnp.expand_dims(scale, 1)).astype(jnp.bfloat16)
        finals.append(lax.all_to_all(narrow, "shard", split_axis=2, concat_axis=1, tiled=True))
        scales.append(
            lax.dynamic_slice_in_dim(scale, lax.axis_index("shard") * width, width, axis=1)
        )
    part_router = (router_weight * router_gain[:, None]).astype(jnp.bfloat16)
    row_router = lax.all_gather(part_router, "shard", axis=0, tiled=True)
    serve_router = lax.all_gather(row_router, "expert", axis=1, tiled=True)
    return (*finals, *scales, serve_router)


def partner(me, k):
    other, bit = me, 1
    while bit <= k:
        if k & bit:
            other = other + bit * (1 - 2 * ((me // bit) % 2))
        bit *= 2
    return other


def kernel(
    n, groups, order,
    mix, mg, sg, mu, su, rw, rg,
    out_g, out_u, sc_g, sc_u, out_r,
    loaded, merged, stage, sums, sums_in, scale_out, scales_in,
    load_sem, small_send, sum_sem, scale_sem, bulk_send, bulk_g, bulk_u, own_sem,
    r_send, r_plane, r_group,
):
    experts, rows, cols = mg.shape
    width = cols // n
    total_rows = rows * n
    me = lax.axis_index("shard")
    group = lax.axis_index("expert")
    sources = (mg, sg, mu, su)

    barrier = pltpu.get_barrier_semaphore()
    for k in range(1, n):
        pl.semaphore_signal(barrier, inc=1, device_id={"shard": partner(me, k)})
    for k in range(1, groups):
        pl.semaphore_signal(barrier, inc=1, device_id={"expert": lax.rem(group + k, groups)})

    def load(e, which=(0, 1, 2, 3)):
        slot = lax.rem(e, LOAD_SLOTS)
        return [
            pltpu.make_async_copy(sources[j].at[e], loaded.at[slot, j], load_sem.at[slot, j])
            for j in which
        ]

    for e in range(min(LOAD_SLOTS, experts)):
        for copy in load(e):
            copy.start()
    pl.semaphore_wait(barrier, n - 1 + groups - 1)

    def remote(src, dst, send, recv, k):
        return pltpu.make_async_remote_copy(
            src_ref=src, dst_ref=dst, send_sem=send, recv_sem=recv,
            device_id={"shard": partner(me, k)},
        )

    def mix_and_sum(e):
        slot, keep = lax.rem(e, LOAD_SLOTS), lax.rem(e, KEPT)
        m = mix[e]
        rest = 1.0 - m
        step = 16
        for t in range(2):
            for copy in load(e, (2 * t, 2 * t + 1)):
                copy.wait()

            def tile(r, acc):
                at = pl.ds(pl.multiple_of(r * step, step), step)
                value = m * loaded[slot, 2 * t, at, :] + rest * loaded[slot, 2 * t + 1, at, :]
                merged[keep, t, at, :] = value
                size = jnp.abs(value)
                return acc + size[:8] + size[8:]

            acc = lax.fori_loop(0, rows // step, tile, jnp.zeros((8, cols), jnp.float32))
            total = jnp.sum(acc, axis=0, keepdims=True)
            for d in range(n):
                sums[e, d, t : t + 1, :] = total[:, d * width : (d + 1) * width]
        sums_in[e, 0] = sums[e, me]
        for k in order:
            remote(sums.at[e, partner(me, k)], sums_in.at[e, k], small_send.at[0], sum_sem.at[e], k).start()

        @pl.when(e + LOAD_SLOTS < experts)
        def _():
            for copy in load(e + LOAD_SLOTS):
                copy.start()

    def settle(e):
        arrived = sums_in.at[e, pl.ds(1, n - 1)]
        pltpu.make_async_copy(arrived, arrived, sum_sem.at[e]).wait()
        scale = jnp.sum(sums_in[e], axis=0) / total_rows
        scale_out[e] = scale
        scales_in[e, 0] = scale
        sc_g[pl.ds(e, 1), :] = scale[0:1]
        sc_u[pl.ds(e, 1), :] = scale[1:2]
        for k in order:
            remote(scale_out.at[e], scales_in.at[e, k], small_send.at[1], scale_sem.at[e], k).start()

    def narrow_and_send(e):
        keep = lax.rem(e, KEPT)
        arrived = scales_in.at[e, pl.ds(1, n - 1)]
        pltpu.make_async_copy(arrived, arrived, scale_sem.at[e]).wait()
        place = pl.ds(pl.multiple_of(me * rows, rows), rows)
        for t, out, sem in ((0, out_g, bulk_g), (1, out_u, bulk_u)):
            for k in (*order, 0):
                at = pl.ds(pl.multiple_of(partner(me, k) * width, width), width)
                scale = scales_in[e, k, t : t + 1, :]
                stage[e, t, k] = (merged[keep, t, :, at] / scale).astype(jnp.bfloat16)
            for k in order:
                remote(stage.at[e, t, k], out.at[e, place], bulk_send.at[t], sem, k).start()
            pltpu.make_async_copy(stage.at[e, t, 0], out.at[e, place], own_sem.at[t]).start()

    height = rw.shape[0]
    high = pl.ds(pl.multiple_of(group * height, height), height)

    def router_plane():
        mine = out_r.at[high, pl.ds(pl.multiple_of(me * rows, rows), rows)]
        mine[...] = (rw[...] * rg[...]).astype(jnp.bfloat16)
        for k in order:
            remote(mine, mine, r_send.at[0], r_plane, k).start()

    def router_groups():
        arrived = out_r.at[high, pl.ds(0, (n - 1) * rows)]
        pltpu.make_async_copy(arrived, arrived, r_plane).wait()
        for k in range(1, groups):
            pltpu.make_async_remote_copy(
                src_ref=out_r.at[high], dst_ref=out_r.at[high],
                send_sem=r_send.at[1], recv_sem=r_group,
                device_id={"expert": lax.rem(group + k, groups)},
            ).start()

    last = experts + SUM_LAG + SCALE_LAG - 1

    @pl.loop(0, last + 1)
    def _(i):
        @pl.when(i < experts)
        def _():
            mix_and_sum(i)

        @pl.when((i >= SUM_LAG) & (i < experts + SUM_LAG))
        def _():
            settle(i - SUM_LAG)

        @pl.when(i >= SUM_LAG + SCALE_LAG)
        def _():
            narrow_and_send(i - SUM_LAG - SCALE_LAG)

        @pl.when(i == SUM_LAG + SCALE_LAG)
        def _():
            router_plane()

        @pl.when(i == last)
        def _():
            router_groups()

    def finish(ref, sem):
        pltpu.make_async_copy(ref, ref, sem).wait()

    others = pl.ds(0, (n - 1) * rows)
    for t, half in enumerate((sums_in, scales_in)):
        finish(half.at[:, pl.ds(1, n - 1)], small_send.at[t])
    finish(out_r.at[pl.ds(0, height), others], r_send.at[0])
    if groups > 1:
        for sem in (r_send.at[1], r_group):
            finish(out_r.at[pl.ds(0, (groups - 1) * height)], sem)
    for t, (out, sem) in enumerate(((out_g, bulk_g), (out_u, bulk_u))):
        finish(out.at[:, others], bulk_send.at[t])
        finish(out.at[:, pl.ds(0, rows)], own_sem.at[t])
        finish(out.at[:, others], sem)


def fused(n, groups, master_gate, second_gate, master_up, second_up, mix_share, router_weight, router_gain):
    experts, rows, cols = master_gate.shape
    width = cols // n
    per_group = router_weight.shape[1]
    order = sorted(range(1, n), key=lambda k: (k // 2 == 0, -bin(k // 2).count("1"), k % 2, k))
    f32, bf16 = jnp.float32, jnp.bfloat16
    final = jax.ShapeDtypeStruct((experts, rows * n, width), bf16)
    scale = jax.ShapeDtypeStruct((experts, width), f32)
    anywhere = pl.BlockSpec(memory_space=pl.ANY)
    vmem = pl.BlockSpec(memory_space=pltpu.VMEM)
    final_gate, final_up, scale_gate, scale_up, router = pl.pallas_call(
        functools.partial(kernel, n, groups, order),
        out_shape=(
            final, final, scale, scale,
            jax.ShapeDtypeStruct((groups * per_group, n * rows), bf16),
        ),
        in_specs=[pl.BlockSpec(memory_space=pltpu.SMEM)] + [anywhere] * 4 + [vmem] * 2,
        out_specs=(anywhere, anywhere, vmem, vmem, vmem),
        scratch_shapes=[
            pltpu.VMEM((LOAD_SLOTS, 4, rows, cols), f32),
            pltpu.VMEM((KEPT, 2, rows, cols), f32),
            pltpu.VMEM((experts, 2, n, rows, width), bf16),
            pltpu.VMEM((experts, n, 2, width), f32),
            pltpu.VMEM((experts, n, 2, width), f32),
            pltpu.VMEM((experts, 2, width), f32),
            pltpu.VMEM((experts, n, 2, width), f32),
            pltpu.SemaphoreType.DMA((LOAD_SLOTS, 4)),
            pltpu.SemaphoreType.DMA((2,)),
            pltpu.SemaphoreType.DMA((experts,)),
            pltpu.SemaphoreType.DMA((experts,)),
            pltpu.SemaphoreType.DMA((2,)),
            pltpu.SemaphoreType.DMA,
            pltpu.SemaphoreType.DMA,
            pltpu.SemaphoreType.DMA((2,)),
            pltpu.SemaphoreType.DMA((2,)),
            pltpu.SemaphoreType.DMA,
            pltpu.SemaphoreType.DMA,
        ],
        compiler_params=pltpu.CompilerParams(
            collective_id=0, has_side_effects=True, vmem_limit_bytes=60 * 1024 * 1024
        ),
    )(
        mix_share, master_gate, second_gate, master_up, second_up,
        router_weight.T, router_gain[None, :],
    )
    return final_gate, final_up, scale_gate, scale_up, router.T


def solution(mesh):
    n, groups = mesh.shape["shard"], mesh.shape["expert"]

    def local(master_gate, *rest):
        width = master_gate.shape[2] // n
        whole_lanes = width % LANES == 0 and n & (n - 1) == 0 and n > 1 and master_gate.shape[1] % 16 == 0
        if whole_lanes:
            return fused(n, groups, master_gate, *rest)
        return plain(width, master_gate, *rest)

    return jax.shard_map(
        local,
        mesh=mesh,
        in_specs=(
            P("expert", "shard", None),
            P("expert", "shard", None),
            P("expert", "shard", None),
            P("expert", "shard", None),
            P("expert"),
            P("shard", "expert"),
            P("shard"),
        ),
        out_specs=(
            P("expert", None, "shard"),
            P("expert", None, "shard"),
            P("expert", "shard"),
            P("expert", "shard"),
            P(),
        ),
        check_vma=False,
    )
```

```python
import functools

import jax
import jax.numpy as jnp
from jax import lax
from jax.experimental import pallas as pl
from jax.experimental.pallas import tpu as pltpu
from jax.sharding import PartitionSpec as P

LANES = 128
LOAD_SLOTS = 3
SUM_LAG = 1
SCALE_LAG = 1
KEPT = SUM_LAG + SCALE_LAG + 1


def plain(width, master_gate, second_gate, master_up, second_up, mix_share, router_weight, router_gain):
    share = mix_share[:, None, None]
    merged_gate = share * master_gate + (1.0 - share) * second_gate
    merged_up = share * master_up + (1.0 - share) * second_up
    total_gate, total_up = lax.psum(
        (jnp.sum(jnp.abs(merged_gate), axis=1), jnp.sum(jnp.abs(merged_up), axis=1)), "shard"
    )
    rows = master_gate.shape[1] * lax.axis_size("shard")
    finals, scales = [], []
    for merged, total in ((merged_gate, total_gate), (merged_up, total_up)):
        scale = total / rows
        narrow = (merged / jnp.expand_dims(scale, 1)).astype(jnp.bfloat16)
        finals.append(lax.all_to_all(narrow, "shard", split_axis=2, concat_axis=1, tiled=True))
        scales.append(
            lax.dynamic_slice_in_dim(scale, lax.axis_index("shard") * width, width, axis=1)
        )
    part_router = (router_weight * router_gain[:, None]).astype(jnp.bfloat16)
    row_router = lax.all_gather(part_router, "shard", axis=0, tiled=True)
    serve_router = lax.all_gather(row_router, "expert", axis=1, tiled=True)
    return (*finals, *scales, serve_router)


def partner(me, k):
    other, bit = me, 1
    while bit <= k:
        if k & bit:
            other = other + bit * (1 - 2 * ((me // bit) % 2))
        bit *= 2
    return other


def kernel(
    n, groups, order,
    mix, mg, sg, mu, su, rw, rg,
    out_g, out_u, sc_g, sc_u, out_r,
    loaded, merged, stage, sums, sums_in, scale_out, scales_in,
    load_sem, small_send, sum_sem, scale_sem, bulk_send, bulk_g, bulk_u,
    r_send, r_plane, r_group,
):
    experts, rows, cols = mg.shape
    width = cols // n
    total_rows = rows * n
    me = lax.axis_index("shard")
    group = lax.axis_index("expert")
    sources = (mg, sg, mu, su)

    barrier = pltpu.get_barrier_semaphore()
    for k in range(1, n):
        pl.semaphore_signal(barrier, inc=1, device_id={"shard": partner(me, k)})
    for k in range(1, groups):
        pl.semaphore_signal(barrier, inc=1, device_id={"expert": lax.rem(group + k, groups)})

    def load(e, which=(0, 1, 2, 3)):
        slot = lax.rem(e, LOAD_SLOTS)
        return [
            pltpu.make_async_copy(sources[j].at[e], loaded.at[slot, j], load_sem.at[slot, j])
            for j in which
        ]

    for e in range(min(LOAD_SLOTS, experts)):
        for copy in load(e):
            copy.start()
    pl.semaphore_wait(barrier, n - 1 + groups - 1)

    def remote(src, dst, send, recv, k):
        return pltpu.make_async_remote_copy(
            src_ref=src, dst_ref=dst, send_sem=send, recv_sem=recv,
            device_id={"shard": partner(me, k)},
        )

    def mix_and_sum(e):
        slot, keep = lax.rem(e, LOAD_SLOTS), lax.rem(e, KEPT)
        m = mix[e]
        rest = 1.0 - m
        step = 16
        for t in range(2):
            for copy in load(e, (2 * t, 2 * t + 1)):
                copy.wait()

            def tile(r, acc):
                at = pl.ds(pl.multiple_of(r * step, step), step)
                value = m * loaded[slot, 2 * t, at, :] + rest * loaded[slot, 2 * t + 1, at, :]
                merged[keep, t, at, :] = value
                size = jnp.abs(value)
                return acc + size[:8] + size[8:]

            acc = lax.fori_loop(0, rows // step, tile, jnp.zeros((8, cols), jnp.float32))
            total = jnp.sum(acc, axis=0, keepdims=True)
            for d in range(n):
                sums[e, d, t : t + 1, :] = total[:, d * width : (d + 1) * width]
        sums_in[e, 0] = sums[e, me]
        for k in order:
            remote(sums.at[e, partner(me, k)], sums_in.at[e, k], small_send.at[0], sum_sem.at[e], k).start()

        @pl.when(e + LOAD_SLOTS < experts)
        def _():
            for copy in load(e + LOAD_SLOTS):
                copy.start()

    def settle(e):
        arrived = sums_in.at[e, pl.ds(1, n - 1)]
        pltpu.make_async_copy(arrived, arrived, sum_sem.at[e]).wait()
        scale = jnp.sum(sums_in[e], axis=0) / total_rows
        scale_out[e] = scale
        scales_in[e, 0] = scale
        sc_g[pl.ds(e, 1), :] = scale[0:1]
        sc_u[pl.ds(e, 1), :] = scale[1:2]
        for k in order:
            remote(scale_out.at[e], scales_in.at[e, k], small_send.at[1], scale_sem.at[e], k).start()

    def narrow_and_send(e):
        keep = lax.rem(e, KEPT)
        arrived = scales_in.at[e, pl.ds(1, n - 1)]
        pltpu.make_async_copy(arrived, arrived, scale_sem.at[e]).wait()
        place = pl.ds(pl.multiple_of(me * rows, rows), rows)
        for t, out, sem in ((0, out_g, bulk_g), (1, out_u, bulk_u)):
            for k in (*order, 0):
                at = pl.ds(pl.multiple_of(partner(me, k) * width, width), width)
                scale = scales_in[e, k, t : t + 1, :]
                narrow = (merged[keep, t, :, at] / scale).astype(jnp.bfloat16)
                if k:
                    stage[e, t, k - 1] = narrow
                else:
                    out[e, place, :] = narrow
            for k in order:
                remote(stage.at[e, t, k - 1], out.at[e, place], bulk_send.at[t], sem, k).start()

    height = rw.shape[0]
    high = pl.ds(pl.multiple_of(group * height, height), height)

    def router_plane():
        mine = out_r.at[high, pl.ds(pl.multiple_of(me * rows, rows), rows)]
        mine[...] = (rw[...] * rg[...]).astype(jnp.bfloat16)
        for k in order:
            remote(mine, mine, r_send.at[0], r_plane, k).start()

    def router_groups():
        arrived = out_r.at[high, pl.ds(0, (n - 1) * rows)]
        pltpu.make_async_copy(arrived, arrived, r_plane).wait()
        for k in range(1, groups):
            pltpu.make_async_remote_copy(
                src_ref=out_r.at[high], dst_ref=out_r.at[high],
                send_sem=r_send.at[1], recv_sem=r_group,
                device_id={"expert": lax.rem(group + k, groups)},
            ).start()

    last = experts + SUM_LAG + SCALE_LAG - 1

    @pl.loop(0, last + 1)
    def _(i):
        @pl.when(i < experts)
        def _():
            mix_and_sum(i)

        @pl.when((i >= SUM_LAG) & (i < experts + SUM_LAG))
        def _():
            settle(i - SUM_LAG)

        @pl.when(i >= SUM_LAG + SCALE_LAG)
        def _():
            narrow_and_send(i - SUM_LAG - SCALE_LAG)

        @pl.when(i == SUM_LAG + SCALE_LAG)
        def _():
            router_plane()

        @pl.when(i == last)
        def _():
            router_groups()

    def finish(ref, sem):
        pltpu.make_async_copy(ref, ref, sem).wait()

    others = pl.ds(0, (n - 1) * rows)
    for t, half in enumerate((sums_in, scales_in)):
        finish(half.at[:, pl.ds(1, n - 1)], small_send.at[t])
    finish(out_r.at[pl.ds(0, height), others], r_send.at[0])
    if groups > 1:
        for sem in (r_send.at[1], r_group):
            finish(out_r.at[pl.ds(0, (groups - 1) * height)], sem)
    for t, (out, sem) in enumerate(((out_g, bulk_g), (out_u, bulk_u))):
        finish(out.at[:, others], bulk_send.at[t])
        finish(out.at[:, others], sem)


def fused(n, groups, master_gate, second_gate, master_up, second_up, mix_share, router_weight, router_gain):
    experts, rows, cols = master_gate.shape
    width = cols // n
    per_group = router_weight.shape[1]
    order = sorted(range(1, n), key=lambda k: (k // 2 == 0, -bin(k // 2).count("1"), k % 2, k))
    f32, bf16 = jnp.float32, jnp.bfloat16
    final = pltpu.VMEM((experts, rows * n, width), bf16)
    scale = jax.ShapeDtypeStruct((experts, width), f32)
    anywhere = pl.BlockSpec(memory_space=pl.ANY)
    vmem = pl.BlockSpec(memory_space=pltpu.VMEM)
    final_gate, final_up, scale_gate, scale_up, router = pl.pallas_call(
        functools.partial(kernel, n, groups, order),
        out_shape=(
            final, final, scale, scale,
            jax.ShapeDtypeStruct((groups * per_group, n * rows), bf16),
        ),
        in_specs=[pl.BlockSpec(memory_space=pltpu.SMEM)] + [anywhere] * 4 + [vmem] * 2,
        out_specs=(vmem,) * 5,
        scratch_shapes=[
            pltpu.VMEM((LOAD_SLOTS, 4, rows, cols), f32),
            pltpu.VMEM((KEPT, 2, rows, cols), f32),
            pltpu.VMEM((experts, 2, n - 1, rows, width), bf16),
            pltpu.VMEM((experts, n, 2, width), f32),
            pltpu.VMEM((experts, n, 2, width), f32),
            pltpu.VMEM((experts, 2, width), f32),
            pltpu.VMEM((experts, n, 2, width), f32),
            pltpu.SemaphoreType.DMA((LOAD_SLOTS, 4)),
            pltpu.SemaphoreType.DMA((2,)),
            pltpu.SemaphoreType.DMA((experts,)),
            pltpu.SemaphoreType.DMA((experts,)),
            pltpu.SemaphoreType.DMA((2,)),
            pltpu.SemaphoreType.DMA,
            pltpu.SemaphoreType.DMA,
            pltpu.SemaphoreType.DMA((2,)),
            pltpu.SemaphoreType.DMA,
            pltpu.SemaphoreType.DMA,
        ],
        compiler_params=pltpu.CompilerParams(
            collective_id=0, has_side_effects=True, vmem_limit_bytes=36 * 2**20
        ),
    )(
        mix_share, master_gate, second_gate, master_up, second_up,
        router_weight.T, router_gain[None, :],
    )
    return final_gate, final_up, scale_gate, scale_up, router.T


def solution(mesh):
    n, groups = mesh.shape["shard"], mesh.shape["expert"]

    def local(master_gate, *rest):
        width = master_gate.shape[2] // n
        whole_lanes = width % LANES == 0 and n & (n - 1) == 0 and n > 1 and master_gate.shape[1] % 16 == 0
        if whole_lanes:
            return fused(n, groups, master_gate, *rest)
        return plain(width, master_gate, *rest)

    return jax.shard_map(
        local,
        mesh=mesh,
        in_specs=(
            P("expert", "shard", None),
            P("expert", "shard", None),
            P("expert", "shard", None),
            P("expert", "shard", None),
            P("expert"),
            P("shard", "expert"),
            P("shard"),
        ),
        out_specs=(
            P("expert", None, "shard"),
            P("expert", None, "shard"),
            P("expert", "shard"),
            P("expert", "shard"),
            P(),
        ),
        check_vma=False,
    )
```

```python
import functools

import jax
import jax.numpy as jnp
from jax import lax
from jax.experimental import pallas as pl
from jax.experimental.pallas import tpu as pltpu
from jax.sharding import PartitionSpec as P

LANES = 128
LOAD_SLOTS = 3
SUM_LAG = 1
SCALE_LAG = 1
PIECES = 4
KEPT = SUM_LAG + SCALE_LAG + 1


def plain(width, master_gate, second_gate, master_up, second_up, mix_share, router_weight, router_gain):
    share = mix_share[:, None, None]
    merged_gate = share * master_gate + (1.0 - share) * second_gate
    merged_up = share * master_up + (1.0 - share) * second_up
    total_gate, total_up = lax.psum(
        (jnp.sum(jnp.abs(merged_gate), axis=1), jnp.sum(jnp.abs(merged_up), axis=1)), "shard"
    )
    rows = master_gate.shape[1] * lax.axis_size("shard")
    finals, scales = [], []
    for merged, total in ((merged_gate, total_gate), (merged_up, total_up)):
        scale = total / rows
        narrow = (merged / jnp.expand_dims(scale, 1)).astype(jnp.bfloat16)
        finals.append(lax.all_to_all(narrow, "shard", split_axis=2, concat_axis=1, tiled=True))
        scales.append(
            lax.dynamic_slice_in_dim(scale, lax.axis_index("shard") * width, width, axis=1)
        )
    part_router = (router_weight * router_gain[:, None]).astype(jnp.bfloat16)
    row_router = lax.all_gather(part_router, "shard", axis=0, tiled=True)
    serve_router = lax.all_gather(row_router, "expert", axis=1, tiled=True)
    return (*finals, *scales, serve_router)


def partner(me, k):
    other, bit = me, 1
    while bit <= k:
        if k & bit:
            other = other + bit * (1 - 2 * ((me // bit) % 2))
        bit *= 2
    return other


def kernel(
    n, groups, order,
    mix_at, mg, sg, mu, su, rw_at, rg_at,
    out_g, out_u, sc_g, sc_u, out_r,
    mix, rw, rg, loaded, merged, stage, sums, sums_in, first_in, scale_out, scales_in,
    param_sem, load_sem, small_send, sum_sem, scale_sem, bulk_send, bulk_g, bulk_u,
    r_send, r_plane, r_group,
):
    experts, rows, cols = mg.shape
    width = cols // n
    total_rows = rows * n
    me = lax.axis_index("shard")
    group = lax.axis_index("expert")
    sources = (mg, sg, mu, su)

    barrier = pltpu.get_barrier_semaphore()
    for k in range(1, n):
        pl.semaphore_signal(barrier, inc=1, device_id={"shard": partner(me, k)})
    for k in range(1, groups):
        pl.semaphore_signal(barrier, inc=1, device_id={"expert": lax.rem(group + k, groups)})

    def load(e, which=(0, 1, 2, 3)):
        slot = lax.rem(e, LOAD_SLOTS)
        return [
            pltpu.make_async_copy(sources[j].at[e], loaded.at[slot, j], load_sem.at[slot, j])
            for j in which
        ]

    params = [
        pltpu.make_async_copy(src, dst, param_sem.at[j])
        for j, (src, dst) in enumerate(((mix_at, mix), (rw_at, rw), (rg_at, rg)))
    ]
    params[0].start()
    for copy in load(0):
        copy.start()
    pl.semaphore_wait(barrier, n - 1 + groups - 1)
    for e in range(1, min(LOAD_SLOTS, experts)):
        for copy in load(e):
            copy.start()
    for copy in params[1:]:
        copy.start()
    params[0].wait()

    def remote(src, dst, send, recv, k):
        return pltpu.make_async_remote_copy(
            src_ref=src, dst_ref=dst, send_sem=send, recv_sem=recv,
            device_id={"shard": partner(me, k)},
        )

    def mix_and_sum(e, first=False):
        slot, keep = lax.rem(e, LOAD_SLOTS), lax.rem(e, KEPT)
        m = mix[e]
        rest = 1.0 - m
        step = 16
        for t in range(2):
            for copy in load(e, (2 * t, 2 * t + 1)):
                copy.wait()

            def tile(r, acc):
                at = pl.ds(pl.multiple_of(r * step, step), step)
                value = m * loaded[slot, 2 * t, at, :] + rest * loaded[slot, 2 * t + 1, at, :]
                merged[keep, t, at, :] = value
                size = jnp.abs(value)
                return acc + size[:8] + size[8:]

            acc = lax.fori_loop(0, rows // step, tile, jnp.zeros((8, cols), jnp.float32))
            total = jnp.sum(acc, axis=0, keepdims=True)
            for d in range(n):
                sums[e, d, t : t + 1, :] = total[:, d * width : (d + 1) * width]
        if first:
            first_in[0] = sums[e]
            for k in order:
                remote(sums.at[e], first_in.at[k], small_send.at[2], sum_sem.at[e], k).start()
        else:
            sums_in[e, 0] = sums[e, me]
            for k in order:
                remote(sums.at[e, partner(me, k)], sums_in.at[e, k], small_send.at[0], sum_sem.at[e], k).start()

        @pl.when(e + LOAD_SLOTS < experts)
        def _():
            for copy in load(e + LOAD_SLOTS):
                copy.start()

    def settle(e):
        arrived = sums_in.at[e, pl.ds(1, n - 1)]
        pltpu.make_async_copy(arrived, arrived, sum_sem.at[e]).wait()
        scale = jnp.sum(sums_in[e], axis=0) / total_rows
        scale_out[e] = scale
        scales_in[e, 0] = scale
        sc_g[pl.ds(e, 1), :] = scale[0:1]
        sc_u[pl.ds(e, 1), :] = scale[1:2]
        for k in order:
            remote(scale_out.at[e], scales_in.at[e, k], small_send.at[1], scale_sem.at[e], k).start()

    def settle_first():
        arrived = first_in.at[pl.ds(1, n - 1)]
        pltpu.make_async_copy(arrived, arrived, sum_sem.at[0]).wait()
        first_in[0] = jnp.sum(first_in[...], axis=0) / total_rows
        for k in range(n):
            scales_in[0, k] = first_in[0, partner(me, k)]
        sc_g[0:1, :] = scales_in[0, 0, 0:1, :]
        sc_u[0:1, :] = scales_in[0, 0, 1:2, :]

    def await_scales(e):
        arrived = scales_in.at[e, pl.ds(1, n - 1)]
        pltpu.make_async_copy(arrived, arrived, scale_sem.at[e]).wait()

    def narrow_and_send(e, which=(0, 1)):
        keep = lax.rem(e, KEPT)
        place = pl.ds(pl.multiple_of(me * rows, rows), rows)
        for t in which:
            out, sem = ((out_g, bulk_g), (out_u, bulk_u))[t]
            ready = None
            for k in (*order, 0):
                at = pl.ds(pl.multiple_of(partner(me, k) * width, width), width)
                scale = scales_in[e, k, t : t + 1, :]
                narrow = (merged[keep, t, :, at] / scale).astype(jnp.bfloat16)
                if k:
                    stage[e, t, k - 1] = narrow
                else:
                    out[e, place, :] = narrow
                if ready is not None:
                    ready.start()
                if k:
                    ready = remote(stage.at[e, t, k - 1], out.at[e, place], bulk_send.at[t], sem, k)

    height = rw.shape[0]
    high = pl.ds(pl.multiple_of(group * height, height), height)

    def router_plane():
        for copy in params[1:]:
            copy.wait()
        mine = out_r.at[high, pl.ds(pl.multiple_of(me * rows, rows), rows)]
        mine[...] = (rw[...] * rg[...]).astype(jnp.bfloat16)
        for k in order:
            remote(mine, mine, r_send.at[0], r_plane, k).start()

    def router_groups():
        arrived = out_r.at[high, pl.ds(0, (n - 1) * rows)]
        pltpu.make_async_copy(arrived, arrived, r_plane).wait()
        for k in range(1, groups):
            pltpu.make_async_remote_copy(
                src_ref=out_r.at[high], dst_ref=out_r.at[high],
                send_sem=r_send.at[1], recv_sem=r_group,
                device_id={"expert": lax.rem(group + k, groups)},
            ).start()

    last = experts + SUM_LAG + SCALE_LAG - 1

    mix_and_sum(0, first=True)

    @pl.loop(1, last + 1)
    def _(i):
        @pl.when(i < experts)
        def _():
            mix_and_sum(i)

        @pl.when(i == 1)
        def _():
            settle_first()
            narrow_and_send(0, (0,))

        @pl.when((i >= SUM_LAG + 1) & (i < experts + SUM_LAG))
        def _():
            settle(i - SUM_LAG)

        @pl.when(i == SUM_LAG + SCALE_LAG)
        def _():
            narrow_and_send(0, (1,))

        @pl.when(i > SUM_LAG + SCALE_LAG)
        def _():
            await_scales(i - SUM_LAG - SCALE_LAG)
            narrow_and_send(i - SUM_LAG - SCALE_LAG)

        @pl.when(i == SUM_LAG + SCALE_LAG)
        def _():
            router_plane()

        @pl.when(i == last)
        def _():
            router_groups()

    def finish(ref, sem):
        pltpu.make_async_copy(ref, ref, sem).wait()

    others = pl.ds(0, (n - 1) * rows)
    finish(first_in.at[pl.ds(1, n - 1)], small_send.at[2])
    for t, half in enumerate((sums_in, scales_in)):
        if experts > 1:
            finish(half.at[pl.ds(1, experts - 1), pl.ds(1, n - 1)], small_send.at[t])
    finish(out_r.at[pl.ds(0, height), others], r_send.at[0])
    if groups > 1:
        for sem in (r_send.at[1], r_group):
            finish(out_r.at[pl.ds(0, (groups - 1) * height)], sem)
    for t, (out, sem) in enumerate(((out_g, bulk_g), (out_u, bulk_u))):
        finish(out.at[:, others], bulk_send.at[t])
        finish(out.at[:, others], sem)


def write_out(*refs):
    *pairs, sems = refs
    count = len(pairs) // 2
    copies = []
    for j, (src, dst) in enumerate(zip(pairs[:count], pairs[count:])):
        pieces = PIECES if len(src.shape) == 3 and src.shape[0] % PIECES == 0 else 1
        size = src.shape[0] // pieces
        for p in range(pieces):
            at = pl.ds(p * size, size)
            copies.append(pltpu.make_async_copy(src.at[at], dst.at[at], sems.at[j, p]))
    for copy in copies:
        copy.start()
    for copy in copies:
        copy.wait()


def fused(n, groups, master_gate, second_gate, master_up, second_up, mix_share, router_weight, router_gain):
    experts, rows, cols = master_gate.shape
    width = cols // n
    per_group = router_weight.shape[1]
    order = sorted(range(1, n), key=lambda k: (k // 2 == 0, -bin(k // 2).count("1"), k % 2, k))
    f32, bf16 = jnp.float32, jnp.bfloat16
    in_hbm = functools.partial(pltpu.with_memory_space_constraint, memory_space=pltpu.HBM)
    final = pltpu.VMEM((experts, rows * n, width), bf16)
    scale = pltpu.VMEM((experts, width), f32)
    hbm = pl.BlockSpec(memory_space=pltpu.HBM)
    vmem = pl.BlockSpec(memory_space=pltpu.VMEM)
    results = pl.pallas_call(
        functools.partial(kernel, n, groups, order),
        out_shape=(
            final, final, scale, scale,
            pltpu.VMEM((groups * per_group, n * rows), bf16),
        ),
        in_specs=[hbm] * 7,
        out_specs=(vmem,) * 5,
        scratch_shapes=[
            pltpu.SMEM((experts,), f32),
            pltpu.VMEM((per_group, rows), f32),
            pltpu.VMEM((1, rows), f32),
            pltpu.VMEM((LOAD_SLOTS, 4, rows, cols), f32),
            pltpu.VMEM((KEPT, 2, rows, cols), f32),
            pltpu.VMEM((experts, 2, n - 1, rows, width), bf16),
            pltpu.VMEM((experts, n, 2, width), f32),
            pltpu.VMEM((experts, n, 2, width), f32),
            pltpu.VMEM((n, n, 2, width), f32),
            pltpu.VMEM((experts, 2, width), f32),
            pltpu.VMEM((experts, n, 2, width), f32),
            pltpu.SemaphoreType.DMA((3,)),
            pltpu.SemaphoreType.DMA((LOAD_SLOTS, 4)),
            pltpu.SemaphoreType.DMA((3,)),
            pltpu.SemaphoreType.DMA((experts,)),
            pltpu.SemaphoreType.DMA((experts,)),
            pltpu.SemaphoreType.DMA((2,)),
            pltpu.SemaphoreType.DMA,
            pltpu.SemaphoreType.DMA,
            pltpu.SemaphoreType.DMA((2,)),
            pltpu.SemaphoreType.DMA,
            pltpu.SemaphoreType.DMA,
        ],
        compiler_params=pltpu.CompilerParams(
            collective_id=0, has_side_effects=True, vmem_limit_bytes=36 * 2**20
        ),
    )(
        in_hbm(mix_share), master_gate, second_gate, master_up, second_up,
        in_hbm(router_weight.T), in_hbm(router_gain[None, :]),
    )
    *results, router = pl.pallas_call(
        write_out,
        out_shape=[jax.ShapeDtypeStruct(x.shape, x.dtype) for x in results],
        in_specs=[vmem] * len(results),
        out_specs=[hbm] * len(results),
        scratch_shapes=[pltpu.SemaphoreType.DMA((len(results), PIECES))],
        compiler_params=pltpu.CompilerParams(vmem_limit_bytes=2**20),
    )(*results)
    return (*results, router.T)


def solution(mesh):
    n, groups = mesh.shape["shard"], mesh.shape["expert"]

    def local(master_gate, *rest):
        width = master_gate.shape[2] // n
        whole_lanes = width % LANES == 0 and n & (n - 1) == 0 and n > 1 and master_gate.shape[1] % 16 == 0
        if whole_lanes:
            return fused(n, groups, master_gate, *rest)
        return plain(width, master_gate, *rest)

    return jax.shard_map(
        local,
        mesh=mesh,
        in_specs=(
            P("expert", "shard", None),
            P("expert", "shard", None),
            P("expert", "shard", None),
            P("expert", "shard", None),
            P("expert"),
            P("shard", "expert"),
            P("shard"),
        ),
        out_specs=(
            P("expert", None, "shard"),
            P("expert", None, "shard"),
            P("expert", "shard"),
            P("expert", "shard"),
            P(),
        ),
        check_vma=False,
    )
```
